32 devices in a mesh: ctx: 32 (over z, y, x, core).
Axes of the slice: x: 2, y: 2, z: 4, core: 2. Of those that a mesh axis runs over, the one named last changes fastest.
Arguments:
- query: bfloat16 [4096, 1024], P('ctx'), may hold values from -11 to 11
- key: bfloat16 [4096, 128], P('ctx'), may hold values from -4 to 4
- value: bfloat16 [4096, 128], P('ctx'), may hold values from -4 to 4
- out_grad: bfloat16 [4096, 1024], P('ctx'), may hold values from -4 to 4
- lengths: int32 [32], replicated, may hold values from 1 to 1409, 4096 in all
Outputs:
- attended: bfloat16 [4096, 1024], P('ctx')
- grad_query: bfloat16 [4096, 1024], P('ctx')
- grad_key: bfloat16 [4096, 128], P('ctx')
- grad_value: bfloat16 [4096, 128], P('ctx')
The draws below stay inside these ranges and needn't reach their ends.
Inputs may be any that keep to these rules, and one draw needn't show every extreme that they name: The lengths of the 32 documents in order; they sum to 4096.
All inputs are finite; a program needn't handle non-finite values.
Results may differ from the reference program's by a relative error of at most 0.03.
Values may be sent and summed in bfloat16 or wider, within the bound.
A program may use at most 64 MiB of HBM per device.

```python
import math
import jax
import jax.numpy as jnp
import numpy as np
from jax import lax

HEADS = 8
HD = 128
TOK_DEV = 128
SPAN = 11
TOKENS = 4096
MAXDOC = 1409
NDOCS = 32
N_CTX = 32


def paired_draw(key):
    streams = jax.random.split(jax.random.fold_in(key, 31), 2)
    base_query = jnp.clip(jax.random.normal(streams[0], (TOKENS, HEADS, HD), jnp.float32), -4.0, 4.0)
    base_key = jnp.clip(jax.random.normal(streams[1], (TOKENS, HD), jnp.float32), -4.0, 4.0)
    return (base_query, base_key)


def draw_query(key, part):
    made_query, made_key = paired_draw(key)
    return made_query.reshape(TOKENS, HEADS * HD).astype(jnp.bfloat16)


def draw_key(key, part):
    made_query, made_key = paired_draw(key)
    return made_key.astype(jnp.bfloat16)


def levels(rng, shape, cuts, low, high):
    level = 1.0
    for position, blocks in cuts:
        heights = jax.random.uniform(jax.random.fold_in(jax.random.fold_in(rng, 6), position), (blocks,), jnp.float32, low / len(cuts), high / len(cuts))
        level = level * jnp.repeat(jnp.exp(heights), shape[position] // blocks).reshape((-1,) + (1,) * (len(shape) - 1 - position))
    return level


def profile(count, total, limit, skew):
    portions = [(1 << 20) // math.isqrt(rank ** skew) + 1 for rank in range(2, count + 1)]
    surplus, counts = total - limit - (count - 1), [1] * (count - 1)
    while surplus > 0:
        candidates = [i for i in range(count - 1) if counts[i] < limit]
        mass, remaining = sum([portions[i] for i in candidates]), surplus
        for i in candidates:
            more = min(limit - counts[i], max(1, remaining * portions[i] // mass), surplus)
            counts[i] = counts[i] + more
            surplus = surplus - more
    return np.array([limit] + counts)


def ragged(rng, count, total, most, lean):
    if count == 2:
        one = jax.random.randint(rng, (), max(1, total - most), min(most, total - 1) + 1)
        return jnp.stack([one, total - one])
    tallies = jnp.asarray(profile(count, total, most, lean), jnp.int32)
    twos = (count - 1) // 2
    donor, receiver = tallies[1:1 + 2 * twos:2], tallies[2:2 + 2 * twos:2]
    slack = jnp.minimum(donor - 1, most - receiver)
    shifted = jax.random.randint(jax.random.fold_in(rng, 1), (twos,), 0, 1 << 20) % (slack + 1)
    tallies = tallies.at[1:1 + 2 * twos:2].set(donor - shifted).at[2:2 + 2 * twos:2].set(receiver + shifted)
    return tallies[jax.random.permutation(jax.random.fold_in(rng, 2), count)]


def gaussian(key, extent, width, bound, pieces=(), kind=jnp.bfloat16):
    result = width * jax.random.normal(key, extent, jnp.float32)
    if pieces:
        result = result * levels(key, extent, pieces, -0.22, 0.18)
    return jnp.clip(result, -bound, bound).astype(kind)


def setup_inputs(seed: int = 0) -> dict:
    keys = jax.random.split(jax.random.key(seed), 6)
    query = draw_query(jax.random.fold_in(keys[5], 71), 0)
    key = draw_key(jax.random.fold_in(keys[5], 71), 0)
    value = gaussian(keys[2], (TOKENS, HD), 1.0, 4.0, ((0, 32),))
    out_grad = gaussian(keys[3], (TOKENS, HEADS * HD), 1.0, 4.0, ((0, 32),))
    lengths = ragged(keys[4], NDOCS, TOKENS, MAXDOC, 2).astype(jnp.int32)
    return dict(query=query, key=key, value=value, out_grad=out_grad, lengths=lengths)


def reference(query, key, value, out_grad, lengths):
    scaling = HD ** -0.5
    doc_ends = jnp.cumsum(lengths).astype(jnp.int32)
    doc_starts = jnp.concatenate([jnp.zeros((1,), jnp.int32), doc_ends[:-1]])
    positions = jnp.arange(TOKENS, dtype=jnp.int32)
    doc_index = jnp.searchsorted(doc_ends, positions, side="right").astype(jnp.int32)
    starts = doc_starts[doc_index].astype(jnp.int32)
    margin = SPAN * TOK_DEV
    window_len = (SPAN + 1) * TOK_DEV
    padded_key = jnp.concatenate([jnp.zeros((margin, HD), key.dtype), key])
    padded_value = jnp.concatenate([jnp.zeros((margin, HD), value.dtype), value])

    def one_block(grads, block):
        first = (block * TOK_DEV).astype(jnp.int32)
        q_block = lax.dynamic_slice_in_dim(query, first, TOK_DEV, 0).reshape(TOK_DEV, HEADS, HD).astype(jnp.float32)
        g_block = lax.dynamic_slice_in_dim(out_grad, first, TOK_DEV, 0).reshape(TOK_DEV, HEADS, HD).astype(jnp.float32)
        k_window = lax.dynamic_slice_in_dim(padded_key, first, window_len, 0).astype(jnp.float32)
        v_window = lax.dynamic_slice_in_dim(padded_value, first, window_len, 0).astype(jnp.float32)
        query_pos = first + jnp.arange(TOK_DEV, dtype=jnp.int32)
        start_block = lax.dynamic_slice_in_dim(starts, first, TOK_DEV, 0)
        key_pos = first - margin + jnp.arange(window_len, dtype=jnp.int32)
        allowed = (key_pos[None, :] >= start_block[:, None]) & (key_pos[None, :] <= query_pos[:, None])
        logits = jnp.einsum("thc,kc->htk", q_block, k_window) * scaling
        logits = jnp.where(allowed[None], logits, -1e30)
        row_max = jnp.max(logits, axis=2)
        expo = jnp.where(allowed[None], jnp.exp(logits - row_max[..., None]), 0.0)
        row_sum = jnp.sum(expo, axis=2)
        probabilities = expo / row_sum[..., None]
        weights = lax.optimization_barrier(probabilities.astype(jnp.bfloat16)).astype(jnp.float32)
        attended = jnp.einsum("htk,kc->thc", weights, v_window).astype(jnp.bfloat16)
        row_dot = jnp.einsum("thc,thc->ht", g_block, attended.astype(jnp.float32))
        grad_probs = jnp.einsum("thc,kc->htk", g_block, v_window)
        grad_scores = probabilities * (grad_probs - row_dot[..., None])
        grad_scores = lax.optimization_barrier(grad_scores.astype(jnp.bfloat16)).astype(jnp.float32)
        grad_query = (scaling * jnp.einsum("htk,kc->thc", grad_scores, k_window)).astype(jnp.bfloat16)
        grad_key = scaling * jnp.einsum("htk,thc->kc", grad_scores, q_block)
        grad_value = jnp.einsum("htk,thc->kc", weights, g_block)
        current = lax.dynamic_slice_in_dim(grads, first, window_len, 1)
        grads = lax.dynamic_update_slice_in_dim(grads, current + jnp.stack([grad_key, grad_value]), first, 1)
        return grads, (attended.reshape(TOK_DEV, HEADS * HD), grad_query.reshape(TOK_DEV, HEADS * HD))

    grads_start = jnp.zeros((2, TOKENS + margin, HD), jnp.float32)
    grads, outputs = lax.scan(one_block, grads_start, jnp.arange(N_CTX, dtype=jnp.int32))
    attended = outputs[0].reshape(TOKENS, HEADS * HD)
    grad_query = outputs[1].reshape(TOKENS, HEADS * HD)
    return attended, grad_query, grads[0, margin:].astype(jnp.bfloat16), grads[1, margin:].astype(jnp.bfloat16)
```

```python
import functools

import jax
import jax.numpy as jnp
from jax import lax
from jax.experimental import pallas as pl
from jax.experimental.pallas import tpu as pltpu
from jax.sharding import PartitionSpec as P

SPAN = 11
SLOTS = SPAN + 1
GROUP = 8
LOG2E = 1.4426950408889634
MESH = pl.DeviceIdType.MESH

FORWARD_CHUNKS = ((0,), (8, 2), (4, 6), (1, 3), (5, 7), (10, 9), (11,))
BACKWARD_ORDER = (10, 2, 0, 4, 6, 8)


def contract(a, b, dims):
    return lax.dot_general(a, b, (dims, ((), ())), preferred_element_type=jnp.float32)


def kernel(
    count,
    lengths, query, key, value, out_grad,
    attended, grad_query, grad_key, grad_value,
    q, g, g_t, kv, e_all, dp_all, m_slot, m_run, l_run, o_t, dq_t,
    part, outbox, partner_in, own_in, fwd_in, far_in, att_buf, dq_buf, dkv_buf,
    load_sem, recv_sem, send_sem, grad_recv, grad_send, out_sem,
):
    tok = key.shape[0]
    hd = key.shape[1]
    heads = query.shape[1] // hd
    wide = 2 * hd
    rows = heads * tok
    pairs = heads // 2
    scale = hd ** -0.5
    me = lax.axis_index("ctx")
    place = lax.rem(me, GROUP)
    chip = place // 2
    odd = lax.rem(me, 2)
    is_even = odd == 0
    is_odd = odd == 1
    partner = me + 1 - 2 * odd
    chips = GROUP // 2

    loads = [
        pltpu.make_async_copy(key, kv.at[0, 0], load_sem.at[0]),
        pltpu.make_async_copy(value, kv.at[0, 1], load_sem.at[1]),
    ]
    for h in range(heads):
        cols = pl.ds(h * hd, hd)
        at = pl.ds(h * tok, tok)
        loads.append(pltpu.make_async_copy(query.at[:, cols], q.at[at, :], load_sem.at[2 + 2 * h]))
        loads.append(pltpu.make_async_copy(out_grad.at[:, cols], g.at[at, :], load_sem.at[3 + 2 * h]))
    for copy in loads:
        copy.start()

    greet = [(partner, None)]
    for dh in range(1, chips):
        greet.append((me + 2 * dh, chip + dh < chips))
        greet.append((me - 2 * dh, chip - dh >= 0))
    greet.append((me + 2, (chip == chips - 1) & (me + 2 < count)))
    greet.append((me - 2, (chip == 0) & (me - 2 >= 0)))
    greet.append((me + GROUP, me + GROUP < count))
    greet.append((me - GROUP, me - GROUP >= 0))
    greet.append((me + 3, is_odd & (me + 3 < count)))
    greet.append((me - 3, is_even & (me - 3 >= 0)))
    barrier = pltpu.get_barrier_semaphore()
    total = jnp.int32(1)
    for device, there in greet:
        if there is None:
            pl.semaphore_signal(barrier, inc=1, device_id=(device,), device_id_type=MESH)
        else:
            @pl.when(there)
            def _(device=device):
                pl.semaphore_signal(barrier, inc=1, device_id=(device,), device_id_type=MESH)
            total = total + there.astype(jnp.int32)
    loads[0].wait()
    loads[1].wait()
    pl.semaphore_wait(barrier, total)

    sent = []

    def send(src, dst, ssem, rsem, device, there):
        copy = pltpu.make_async_remote_copy(
            src_ref=src, dst_ref=dst, send_sem=ssem, recv_sem=rsem,
            device_id=(device,), device_id_type=MESH)

        @pl.when(there)
        def _():
            copy.start()
        sent.append((copy, there))

    n_send = [0]

    def send_slot(slot, dst_slot, device, there):
        k = n_send[0]
        n_send[0] += 1
        send(kv.at[slot], kv.at[dst_slot], send_sem.at[k], recv_sem.at[dst_slot], device, there)

    def arrive(slot):
        @pl.when(me >= slot)
        def _():
            pltpu.make_async_remote_copy(
                src_ref=kv.at[slot], dst_ref=kv.at[slot], send_sem=send_sem.at[0],
                recv_sem=recv_sem.at[slot], device_id=(partner,), device_id_type=MESH).wait_recv()

    def relay(slot):
        arrive(slot)
        send_slot(slot, slot + 1 - 2 * odd, partner, me >= slot)

    send_slot(0, GROUP, me + GROUP, me + GROUP < count)
    send_slot(0, 1, partner, is_even)
    for dh in range(1, chips):
        send_slot(0, 2 * dh, me + 2 * dh, chip + dh < chips)

    for slot in range(1, SLOTS):
        @pl.when(me < slot)
        def _(slot=slot):
            kv[slot] = jnp.zeros_like(kv[slot])
    lane_pos = me * tok + lax.broadcasted_iota(jnp.int32, (1, tok), 1)

    def doc_step(d, carry):
        end, start = carry
        end = end + lengths[d]
        return end, jnp.where(end <= lane_pos, end, start)

    _, start = lax.fori_loop(
        0, lengths.shape[0], doc_step, (jnp.int32(0), jnp.zeros((1, tok), jnp.int32)))
    for copy in loads[2:]:
        copy.wait()
    for h in range(heads):
        at = pl.ds(h * tok, tok)
        g_t[:, at] = jnp.transpose(g[at, :].astype(jnp.float32))

    def forward(slots, first):
        biases = []
        for slot in slots:
            key_pos = (me - slot) * tok + lax.broadcasted_iota(jnp.int32, (tok, 1), 0)
            seen = key_pos >= start
            if slot == 0:
                seen = seen & (key_pos <= lane_pos)
            biases.append(jnp.where(seen, 0.0, -1e30).astype(jnp.float32))
        bias = jnp.concatenate(biases, 0) if len(slots) > 1 else biases[0]
        bias = jnp.concatenate([bias, bias], 1)
        kb = jnp.concatenate([kv[s, 0] for s in slots], 0)
        vb = jnp.concatenate([kv[s, 1] for s in slots], 0)
        for hp in range(pairs):
            at = pl.ds(hp * 2 * tok, 2 * tok)
            s = contract(kb, q[at, :], ((1,), (1,))) * (scale * LOG2E) + bias
            dp = contract(vb, g[at, :], ((1,), (1,)))
            top = jnp.max(s, axis=0, keepdims=True)
            if not first:
                old = m_run[:, at]
                top = jnp.maximum(old, top)
            e = jnp.exp2(s - top)
            fresh = jnp.sum(e, axis=0, keepdims=True)
            o = contract(vb, e.astype(jnp.bfloat16), ((0,), (0,)))
            if first:
                l_run[:, at] = fresh
                o_t[:, at] = o
            else:
                alpha = jnp.exp2(old - top)
                l_run[:, at] = l_run[:, at] * alpha + fresh
                o_t[:, at] = o_t[:, at] * alpha + o
            m_run[:, at] = top
            for n, slot in enumerate(slots):
                e_all[slot, :, at] = e[n * tok:(n + 1) * tok]
                dp_all[slot, :, at] = dp[n * tok:(n + 1) * tok]
                m_slot[slot, :, at] = top

    forward((0,), True)
    arrive(GROUP)
    have = me >= GROUP
    send_slot(GROUP, GROUP + 2, me + 2, have & (me + 2 < count))
    for dh in range(1, chips):
        send_slot(GROUP, GROUP - 2 * dh, me - 2 * dh, have & (chip - dh >= 0))
    send_slot(GROUP, GROUP + 3, me + 3, have & is_odd & (me + 3 < count))
    send_slot(GROUP, GROUP + 1 - 2 * odd, partner, have)
    relay(2)
    forward((8, 2), False)
    relay(4)
    relay(6)
    forward((4, 6), False)
    relay(10)
    arrive(1)
    arrive(3)
    forward((1, 3), False)
    arrive(5)
    arrive(7)
    forward((5, 7), False)
    arrive(9)
    forward((10, 9), False)
    arrive(11)
    forward((11,), False)

    inv = 1.0 / l_run[...]
    att = (o_t[...] * inv).astype(jnp.bfloat16).astype(jnp.float32)
    o_t[...] = att
    row_dot = jnp.sum(g_t[...] * att, axis=0, keepdims=True)
    m_end = m_run[...]

    def chunk(i):
        e_slot = BACKWARD_ORDER[i]
        o_slot = lax.rem(e_slot + 2 * odd - 1 + SLOTS, SLOTS)
        slots = (e_slot, o_slot)
        kb = jnp.concatenate([kv[s, 0] for s in slots], 0)
        dk = jnp.zeros((2 * tok, hd), jnp.float32)
        dv = jnp.zeros((2 * tok, hd), jnp.float32)
        for hp in range(pairs):
            lo = hp * 2 * tok
            at = pl.ds(lo, 2 * tok)
            dot = row_dot[:, lo:lo + 2 * tok]
            ps, dss = [], []
            for s in slots:
                f = jnp.exp2(m_slot[s, :, at] - m_end[:, lo:lo + 2 * tok]) * inv[:, lo:lo + 2 * tok]
                p = e_all[s, :, at] * f
                dss.append((p * (dp_all[s, :, at] - dot)).astype(jnp.bfloat16))
                ps.append(p.astype(jnp.bfloat16))
            p = jnp.concatenate(ps, 0)
            ds = jnp.concatenate(dss, 0)
            dv = dv + contract(p, g[at, :], ((1,), (0,)))
            dk = dk + contract(ds, q[at, :], ((1,), (0,)))
            dq = contract(kb, ds, ((0,), (0,)))
            if i == 0:
                dq_t[:, at] = dq
            else:
                dq_t[:, at] = dq_t[:, at] + dq
        dk = dk * scale
        k = e_slot // 2
        part[k, 0] = dk[:tok]
        part[k, 1] = dv[:tok]
        outbox[k, 0] = dk[tok:].astype(jnp.bfloat16)
        outbox[k, 1] = dv[tok:].astype(jnp.bfloat16)
        if e_slot == 0:
            send(outbox.at[k], partner_in.at[0], grad_send.at[0], grad_recv.at[0], partner, is_odd)
            send(outbox.at[k], far_in.at[1], grad_send.at[1], grad_recv.at[15], me - 3,
                 is_even & (me >= SPAN))
        else:
            send(outbox.at[k], partner_in.at[k], grad_send.at[1 + k], grad_recv.at[k], partner,
                 me >= o_slot)

    def take(ref, sem, there, base):
        @pl.when(there)
        def _():
            pltpu.make_async_remote_copy(
                src_ref=ref, dst_ref=ref, send_sem=grad_send.at[0], recv_sem=sem,
                device_id=(partner,), device_id_type=MESH).wait_recv()
            part[base] = part[base] + ref[...].astype(jnp.float32)

    def up(e_slot):
        k = e_slot // 2
        take(partner_in.at[k], grad_recv.at[k], me >= e_slot, k)
        outbox[SLOTS // 2 + k] = part[k].astype(jnp.bfloat16)
        box = outbox.at[SLOTS // 2 + k]
        near = chip - k >= 0
        if e_slot < GROUP:
            send(box, own_in.at[k - 1], grad_send.at[6 + k], grad_recv.at[5 + k], me - e_slot, near)
            send(box, fwd_in.at[k - 1], grad_send.at[9 + k], grad_recv.at[8 + k],
                 me + GROUP - e_slot, jnp.logical_not(near) & (me >= e_slot))
        else:
            send(box, fwd_in.at[3], grad_send.at[13], grad_recv.at[12], me - 2, me >= e_slot)

    chunk(0)
    chunk(1)
    up(10)
    chunk(2)
    up(2)
    chunk(3)
    chunk(4)
    up(4)
    chunk(5)
    up(6)

    k8 = GROUP // 2
    take(partner_in.at[k8], grad_recv.at[k8], have, k8)
    take(fwd_in.at[3], grad_recv.at[12], have & (me + 2 < count), k8)
    take(far_in.at[1], grad_recv.at[15], have & is_odd & (me + 3 < count), k8)
    for k in (3, 2, 1):
        take(fwd_in.at[k - 1], grad_recv.at[8 + k], have & (chip - (k8 - k) >= 0), k8)
    outbox[SLOTS // 2 + k8] = part[k8].astype(jnp.bfloat16)
    send(outbox.at[SLOTS // 2 + k8], far_in.at[0], grad_send.at[14], grad_recv.at[13],
         me - GROUP, have)

    for h in range(heads):
        at = pl.ds(h * tok, tok)
        cols = pl.ds(h * hd, hd)
        att_buf[:, cols] = jnp.transpose(o_t[:, at]).astype(jnp.bfloat16)
        dq_buf[:, cols] = jnp.transpose(dq_t[:, at] * scale).astype(jnp.bfloat16)
    outs = [
        pltpu.make_async_copy(att_buf, attended, out_sem.at[0]),
        pltpu.make_async_copy(dq_buf, grad_query, out_sem.at[1]),
    ]
    for copy in outs:
        copy.start()

    take(partner_in.at[0], grad_recv.at[0], is_even, 0)
    for k in range(1, chips):
        take(own_in.at[k - 1], grad_recv.at[5 + k], chip + k < chips, 0)
    take(far_in.at[0], grad_recv.at[13], me + GROUP < count, 0)
    dkv_buf[...] = part[0].astype(jnp.bfloat16)
    last = [
        pltpu.make_async_copy(dkv_buf.at[0], grad_key, out_sem.at[2]),
        pltpu.make_async_copy(dkv_buf.at[1], grad_value, out_sem.at[3]),
    ]
    for copy in last:
        copy.start()
    for copy, there in sent:
        @pl.when(there)
        def _(copy=copy):
            copy.wait_send()
    for copy in outs + last:
        copy.wait()


def body(count, query, key, value, out_grad, lengths):
    tok, hd = key.shape
    heads = query.shape[1] // hd
    rows = heads * tok
    half = SLOTS // 2
    any_space = pl.BlockSpec(memory_space=pl.ANY)
    f32, bf16 = jnp.float32, jnp.bfloat16
    dma = pltpu.SemaphoreType.DMA
    scratch = [
        pltpu.VMEM((rows, hd), bf16),
        pltpu.VMEM((rows, hd), bf16),
        pltpu.VMEM((hd, rows), f32),
        pltpu.VMEM((SLOTS, 2, tok, hd), bf16),
        pltpu.VMEM((SLOTS, tok, rows), f32),
        pltpu.VMEM((SLOTS, tok, rows), f32),
        pltpu.VMEM((SLOTS, 1, rows), f32),
        pltpu.VMEM((1, rows), f32),
        pltpu.VMEM((1, rows), f32),
        pltpu.VMEM((hd, rows), f32),
        pltpu.VMEM((hd, rows), f32),
        pltpu.VMEM((half, 2, tok, hd), f32),
        pltpu.VMEM((2 * half, 2, tok, hd), bf16),
        pltpu.VMEM((half, 2, tok, hd), bf16),
        pltpu.VMEM((3, 2, tok, hd), bf16),
        pltpu.VMEM((4, 2, tok, hd), bf16),
        pltpu.VMEM((2, 2, tok, hd), bf16),
        pltpu.VMEM((tok, rows * hd // tok), bf16),
        pltpu.VMEM((tok, rows * hd // tok), bf16),
        pltpu.VMEM((2, tok, hd), bf16),
        dma((2 + 2 * heads,)),
        dma((SLOTS,)),
        dma((24,)),
        dma((16,)),
        dma((16,)),
        dma((4,)),
    ]
    return pl.pallas_call(
        functools.partial(kernel, count),
        out_shape=[
            jax.ShapeDtypeStruct(query.shape, bf16),
            jax.ShapeDtypeStruct(query.shape, bf16),
            jax.ShapeDtypeStruct(key.shape, bf16),
            jax.ShapeDtypeStruct(key.shape, bf16),
        ],
        in_specs=[pl.BlockSpec(memory_space=pltpu.SMEM)] + [any_space] * 4,
        out_specs=[any_space] * 4,
        scratch_shapes=scratch,
        compiler_params=pltpu.CompilerParams(
            collective_id=0, has_side_effects=True, vmem_limit_bytes=40 * 1024 * 1024),
        name="packed_attention",
    )(lengths, query, key, value, out_grad)


def solution(mesh):
    count = mesh.shape["ctx"]
    row = P("ctx", None)
    return jax.shard_map(
        functools.partial(body, count),
        mesh=mesh,
        in_specs=(row, row, row, row, P()),
        out_specs=(row, row, row, row),
        check_vma=False,
    )
```

```python
import functools

import jax
import jax.numpy as jnp
from jax import lax
from jax.experimental import pallas as pl
from jax.experimental.pallas import tpu as pltpu
from jax.sharding import PartitionSpec as P

SPAN = 11
SLOTS = SPAN + 1
GROUP = 8
LOG2E = 1.4426950408889634
MESH = pl.DeviceIdType.MESH

FORWARD_CHUNKS = ((0,), (8, 2), (4, 6), (1, 3), (5, 7), (10, 9), (11,))
BACKWARD_ORDER = (10, 2, 0, 4, 6, 8)


def contract(a, b, dims):
    return lax.dot_general(a, b, (dims, ((), ())), preferred_element_type=jnp.float32)


def kernel(
    count,
    lengths, query, key, value, out_grad,
    attended, grad_query, grad_key, grad_value,
    q, g, g_t, kv, e_all, dp_all, m_slot, m_run, l_run, o_t, dq_t,
    part, outbox, partner_in, own_in, fwd_in, far_in,
    load_sem, recv_sem, send_sem, grad_recv, grad_send,
):
    tok = key.shape[0]
    hd = key.shape[1]
    heads = query.shape[1] // hd
    wide = 2 * hd
    rows = heads * tok
    pairs = heads // 2
    scale = hd ** -0.5
    me = lax.axis_index("ctx")
    place = lax.rem(me, GROUP)
    chip = place // 2
    odd = lax.rem(me, 2)
    is_even = odd == 0
    is_odd = odd == 1
    partner = me + 1 - 2 * odd
    chips = GROUP // 2

    loads = [
        pltpu.make_async_copy(key, kv.at[0, 0], load_sem.at[0]),
        pltpu.make_async_copy(value, kv.at[0, 1], load_sem.at[1]),
    ]
    for h in range(heads):
        cols = pl.ds(h * hd, hd)
        at = pl.ds(h * tok, tok)
        loads.append(pltpu.make_async_copy(query.at[:, cols], q.at[at, :], load_sem.at[2 + 2 * h]))
        loads.append(pltpu.make_async_copy(out_grad.at[:, cols], g.at[at, :], load_sem.at[3 + 2 * h]))
    for copy in loads:
        copy.start()

    greet = [(partner, None)]
    for dh in range(1, chips):
        greet.append((me + 2 * dh, chip + dh < chips))
        greet.append((me - 2 * dh, chip - dh >= 0))
    greet.append((me + 2, (chip == chips - 1) & (me + 2 < count)))
    greet.append((me - 2, (chip == 0) & (me - 2 >= 0)))
    greet.append((me + GROUP, me + GROUP < count))
    greet.append((me - GROUP, me - GROUP >= 0))
    greet.append((me + 3, is_odd & (me + 3 < count)))
    greet.append((me - 3, is_even & (me - 3 >= 0)))
    barrier = pltpu.get_barrier_semaphore()
    total = jnp.int32(1)
    for device, there in greet:
        if there is None:
            pl.semaphore_signal(barrier, inc=1, device_id=(device,), device_id_type=MESH)
        else:
            @pl.when(there)
            def _(device=device):
                pl.semaphore_signal(barrier, inc=1, device_id=(device,), device_id_type=MESH)
            total = total + there.astype(jnp.int32)
    loads[0].wait()
    loads[1].wait()
    pl.semaphore_wait(barrier, total)

    sent = []

    def send(src, dst, ssem, rsem, device, there):
        copy = pltpu.make_async_remote_copy(
            src_ref=src, dst_ref=dst, send_sem=ssem, recv_sem=rsem,
            device_id=(device,), device_id_type=MESH)

        @pl.when(there)
        def _():
            copy.start()
        sent.append((copy, there))

    n_send = [0]

    def send_slot(slot, dst_slot, device, there):
        k = n_send[0]
        n_send[0] += 1
        send(kv.at[slot], kv.at[dst_slot], send_sem.at[k], recv_sem.at[dst_slot], device, there)

    def arrive(slot):
        @pl.when(me >= slot)
        def _():
            pltpu.make_async_remote_copy(
                src_ref=kv.at[slot], dst_ref=kv.at[slot], send_sem=send_sem.at[0],
                recv_sem=recv_sem.at[slot], device_id=(partner,), device_id_type=MESH).wait_recv()

    def relay(slot):
        arrive(slot)
        send_slot(slot, slot + 1 - 2 * odd, partner, me >= slot)

    send_slot(0, GROUP, me + GROUP, me + GROUP < count)
    send_slot(0, 1, partner, is_even)
    for dh in range(1, chips):
        send_slot(0, 2 * dh, me + 2 * dh, chip + dh < chips)

    for slot in range(1, SLOTS):
        @pl.when(me < slot)
        def _(slot=slot):
            kv[slot] = jnp.zeros_like(kv[slot])
    lane_pos = me * tok + lax.broadcasted_iota(jnp.int32, (1, tok), 1)

    def doc_step(d, carry):
        end, start = carry
        end = end + lengths[d]
        return end, jnp.where(end <= lane_pos, end, start)

    _, start = lax.fori_loop(
        0, lengths.shape[0], doc_step, (jnp.int32(0), jnp.zeros((1, tok), jnp.int32)))
    for copy in loads[2:]:
        copy.wait()
    for h in range(heads):
        at = pl.ds(h * tok, tok)
        g_t[:, at] = jnp.transpose(g[at, :].astype(jnp.float32))

    def forward(slots, first):
        biases = []
        for slot in slots:
            key_pos = (me - slot) * tok + lax.broadcasted_iota(jnp.int32, (tok, 1), 0)
            seen = key_pos >= start
            if slot == 0:
                seen = seen & (key_pos <= lane_pos)
            biases.append(jnp.where(seen, 0.0, -1e30).astype(jnp.float32))
        bias = jnp.concatenate(biases, 0) if len(slots) > 1 else biases[0]
        bias = jnp.concatenate([bias, bias], 1)
        kb = jnp.concatenate([kv[s, 0] for s in slots], 0)
        vb = jnp.concatenate([kv[s, 1] for s in slots], 0)
        for hp in range(pairs):
            at = pl.ds(hp * 2 * tok, 2 * tok)
            s = contract(kb, q[at, :], ((1,), (1,))) * (scale * LOG2E) + bias
            dp = contract(vb, g[at, :], ((1,), (1,)))
            top = jnp.max(s, axis=0, keepdims=True)
            if not first:
                old = m_run[:, at]
                top = jnp.maximum(old, top)
            e = jnp.exp2(s - top)
            fresh = jnp.sum(e, axis=0, keepdims=True)
            o = contract(vb, e.astype(jnp.bfloat16), ((0,), (0,)))
            if first:
                l_run[:, at] = fresh
                o_t[:, at] = o
            else:
                alpha = jnp.exp2(old - top)
                l_run[:, at] = l_run[:, at] * alpha + fresh
                o_t[:, at] = o_t[:, at] * alpha + o
            m_run[:, at] = top
            for n, slot in enumerate(slots):
                e_all[slot, :, at] = e[n * tok:(n + 1) * tok]
                dp_all[slot, :, at] = dp[n * tok:(n + 1) * tok]
                m_slot[slot, :, at] = top

    forward((0,), True)
    arrive(GROUP)
    have = me >= GROUP
    send_slot(GROUP, GROUP + 2, me + 2, have & (me + 2 < count))
    for dh in range(1, chips):
        send_slot(GROUP, GROUP - 2 * dh, me - 2 * dh, have & (chip - dh >= 0))
    send_slot(GROUP, GROUP + 3, me + 3, have & is_odd & (me + 3 < count))
    send_slot(GROUP, GROUP + 1 - 2 * odd, partner, have)
    relay(2)
    forward((8, 2), False)
    relay(4)
    relay(6)
    forward((4, 6), False)
    relay(10)
    arrive(1)
    arrive(3)
    forward((1, 3), False)
    arrive(5)
    arrive(7)
    forward((5, 7), False)
    arrive(9)
    forward((10, 9), False)
    arrive(11)
    forward((11,), False)

    inv = 1.0 / l_run[...]
    att = (o_t[...] * inv).astype(jnp.bfloat16).astype(jnp.float32)
    o_t[...] = att
    row_dot = jnp.sum(g_t[...] * att, axis=0, keepdims=True)
    m_end = m_run[...]

    def chunk(i):
        e_slot = BACKWARD_ORDER[i]
        o_slot = lax.rem(e_slot + 2 * odd - 1 + SLOTS, SLOTS)
        slots = (e_slot, o_slot)
        kb = jnp.concatenate([kv[s, 0] for s in slots], 0)
        dk = jnp.zeros((2 * tok, hd), jnp.float32)
        dv = jnp.zeros((2 * tok, hd), jnp.float32)
        for hp in range(pairs):
            lo = hp * 2 * tok
            at = pl.ds(lo, 2 * tok)
            dot = row_dot[:, lo:lo + 2 * tok]
            ps, dss = [], []
            for s in slots:
                f = jnp.exp2(m_slot[s, :, at] - m_end[:, lo:lo + 2 * tok]) * inv[:, lo:lo + 2 * tok]
                p = e_all[s, :, at] * f
                dss.append((p * (dp_all[s, :, at] - dot)).astype(jnp.bfloat16))
                ps.append(p.astype(jnp.bfloat16))
            p = jnp.concatenate(ps, 0)
            ds = jnp.concatenate(dss, 0)
            dv = dv + contract(p, g[at, :], ((1,), (0,)))
            dk = dk + contract(ds, q[at, :], ((1,), (0,)))
            dq = contract(kb, ds, ((0,), (0,)))
            if i == 0:
                dq_t[:, at] = dq
            else:
                dq_t[:, at] = dq_t[:, at] + dq
        dk = dk * scale
        k = e_slot // 2
        part[k, 0] = dk[:tok]
        part[k, 1] = dv[:tok]
        outbox[k, 0] = dk[tok:].astype(jnp.bfloat16)
        outbox[k, 1] = dv[tok:].astype(jnp.bfloat16)
        if e_slot == 0:
            send(outbox.at[k], partner_in.at[0], grad_send.at[0], grad_recv.at[0], partner, is_odd)
            send(outbox.at[k], far_in.at[1], grad_send.at[1], grad_recv.at[15], me - 3,
                 is_even & (me >= SPAN))
        else:
            send(outbox.at[k], partner_in.at[k], grad_send.at[1 + k], grad_recv.at[k], partner,
                 me >= o_slot)

    def take(ref, sem, there, base):
        @pl.when(there)
        def _():
            pltpu.make_async_remote_copy(
                src_ref=ref, dst_ref=ref, send_sem=grad_send.at[0], recv_sem=sem,
                device_id=(partner,), device_id_type=MESH).wait_recv()
            part[base] = part[base] + ref[...].astype(jnp.float32)

    def up(e_slot):
        k = e_slot // 2
        take(partner_in.at[k], grad_recv.at[k], me >= e_slot, k)
        outbox[SLOTS // 2 + k] = part[k].astype(jnp.bfloat16)
        box = outbox.at[SLOTS // 2 + k]
        near = chip - k >= 0
        if e_slot < GROUP:
            send(box, own_in.at[k - 1], grad_send.at[6 + k], grad_recv.at[5 + k], me - e_slot, near)
            send(box, fwd_in.at[k - 1], grad_send.at[9 + k], grad_recv.at[8 + k],
                 me + GROUP - e_slot, jnp.logical_not(near) & (me >= e_slot))
        else:
            send(box, fwd_in.at[3], grad_send.at[13], grad_recv.at[12], me - 2, me >= e_slot)

    chunk(0)
    chunk(1)
    up(10)
    chunk(2)
    up(2)
    chunk(3)
    chunk(4)
    up(4)
    chunk(5)
    up(6)

    k8 = GROUP // 2
    take(partner_in.at[k8], grad_recv.at[k8], have, k8)
    take(fwd_in.at[3], grad_recv.at[12], have & (me + 2 < count), k8)
    take(far_in.at[1], grad_recv.at[15], have & is_odd & (me + 3 < count), k8)
    for k in (3, 2, 1):
        take(fwd_in.at[k - 1], grad_recv.at[8 + k], have & (chip - (k8 - k) >= 0), k8)
    outbox[SLOTS // 2 + k8] = part[k8].astype(jnp.bfloat16)
    send(outbox.at[SLOTS // 2 + k8], far_in.at[0], grad_send.at[14], grad_recv.at[13],
         me - GROUP, have)

    for h in range(heads):
        at = pl.ds(h * tok, tok)
        cols = pl.ds(h * hd, hd)
        attended[:, cols] = jnp.transpose(o_t[:, at]).astype(jnp.bfloat16)
        grad_query[:, cols] = jnp.transpose(dq_t[:, at] * scale).astype(jnp.bfloat16)

    take(partner_in.at[0], grad_recv.at[0], is_even, 0)
    for k in range(1, chips):
        take(own_in.at[k - 1], grad_recv.at[5 + k], chip + k < chips, 0)
    take(far_in.at[0], grad_recv.at[13], me + GROUP < count, 0)
    grad_key[...] = part[0, 0].astype(jnp.bfloat16)
    grad_value[...] = part[0, 1].astype(jnp.bfloat16)
    for copy, there in sent:
        @pl.when(there)
        def _(copy=copy):
            copy.wait_send()


def write_out(a, b, c, d, a_out, b_out, c_out, d_out, sem):
    copies = [
        pltpu.make_async_copy(src, dst, sem.at[i])
        for i, (src, dst) in enumerate(((a, a_out), (b, b_out), (c, c_out), (d, d_out)))
    ]
    for copy in copies:
        copy.start()
    for copy in copies:
        copy.wait()


def body(count, query, key, value, out_grad, lengths):
    tok, hd = key.shape
    heads = query.shape[1] // hd
    rows = heads * tok
    half = SLOTS // 2
    in_hbm = pl.BlockSpec(memory_space=pltpu.HBM)
    f32, bf16 = jnp.float32, jnp.bfloat16
    dma = pltpu.SemaphoreType.DMA
    scratch = [
        pltpu.VMEM((rows, hd), bf16),
        pltpu.VMEM((rows, hd), bf16),
        pltpu.VMEM((hd, rows), f32),
        pltpu.VMEM((SLOTS, 2, tok, hd), bf16),
        pltpu.VMEM((SLOTS, tok, rows), f32),
        pltpu.VMEM((SLOTS, tok, rows), f32),
        pltpu.VMEM((SLOTS, 1, rows), f32),
        pltpu.VMEM((1, rows), f32),
        pltpu.VMEM((1, rows), f32),
        pltpu.VMEM((hd, rows), f32),
        pltpu.VMEM((hd, rows), f32),
        pltpu.VMEM((half, 2, tok, hd), f32),
        pltpu.VMEM((2 * half, 2, tok, hd), bf16),
        pltpu.VMEM((half, 2, tok, hd), bf16),
        pltpu.VMEM((3, 2, tok, hd), bf16),
        pltpu.VMEM((4, 2, tok, hd), bf16),
        pltpu.VMEM((2, 2, tok, hd), bf16),
        dma((2 + 2 * heads,)),
        dma((SLOTS,)),
        dma((24,)),
        dma((16,)),
        dma((16,)),
    ]
    query, key, value, out_grad = [
        pltpu.with_memory_space_constraint(x, pltpu.HBM) for x in (query, key, value, out_grad)]
    results = pl.pallas_call(
        functools.partial(kernel, count),
        out_shape=[
            jax.ShapeDtypeStruct(query.shape, bf16),
            jax.ShapeDtypeStruct(query.shape, bf16),
            jax.ShapeDtypeStruct(key.shape, bf16),
            jax.ShapeDtypeStruct(key.shape, bf16),
        ],
        in_specs=[pl.BlockSpec(memory_space=pltpu.SMEM)] + [in_hbm] * 4,
        out_specs=[pl.BlockSpec(memory_space=pltpu.VMEM)] * 4,
        scratch_shapes=scratch,
        compiler_params=pltpu.CompilerParams(
            collective_id=0, has_side_effects=True, vmem_limit_bytes=40 * 1024 * 1024),
        name="packed_attention",
    )(lengths, query, key, value, out_grad)
    results = [pltpu.with_memory_space_constraint(x, pltpu.VMEM) for x in results]
    return pl.pallas_call(
        write_out,
        out_shape=[jax.ShapeDtypeStruct(r.shape, r.dtype) for r in results],
        in_specs=[pl.BlockSpec(memory_space=pl.ANY)] * 4,
        out_specs=[in_hbm] * 4,
        scratch_shapes=[dma((4,))],
        name="write_out",
    )(*results)


def solution(mesh):
    count = mesh.shape["ctx"]
    row = P("ctx", None)
    return jax.shard_map(
        functools.partial(body, count),
        mesh=mesh,
        in_specs=(row, row, row, row, P()),
        out_specs=(row, row, row, row),
        check_vma=False,
    )
```
